32 devices in a mesh: space: 16 (over z, y, core), tm: 2 (over x).
Axes of the slice: x: 2, y: 2, z: 4, core: 2. Of those that a mesh axis runs over, the one named last changes fastest.
Arguments:
- solutions: bfloat16 [2, 12, 8192, 128], P('tm', None, 'space'), may hold values from -6 to 6
- noise: int32 [2, 64, 12, 8192], P('tm', None, None, 'space'), may hold values from 0 to 3
- momenta: int32 [27, 3], replicated, may hold values from -2 to 2
- pairs: int32 [16, 2], P('tm'), may hold values from 0 to 1
Outputs:
- mesons: float32 [2, 2, 27, 64, 64], P('tm', None, None, 'space')
- correlators: float32 [16, 2, 27], P('tm')
The draws below stay inside these ranges and needn't reach their ends.
All inputs are finite; a program needn't handle non-finite values.
Results may differ from the reference program's by a relative error of at most 0.002.
Values sent between devices are 32-bit elements; how exact they have to be, the bound alone decides.
A program may use at most 64 MiB of HBM per device.

```python
import math
import jax
import jax.numpy as jnp
from jax import lax

NVEC = 64
SPINCOL = 12
MOMS = 27
EXTENT = 48
SITES = 8192
TSL = 2
NPAIRS = 16


def plant(drawn, rng, least, top_value):
    place = [jax.random.randint(jax.random.fold_in(rng, axis), (), 0, length) for axis, length in enumerate(drawn.shape)]
    main_axis = drawn.shape.index(max(drawn.shape))
    next_to = place[:main_axis] + [(place[main_axis] + 1) % drawn.shape[main_axis]] + place[main_axis + 1:]
    return drawn.at[tuple(place)].set(least).at[tuple(next_to)].set(top_value)


def level_of(key, extent, cuts, least, top_value):
    gain, own = 1.0, jax.random.fold_in(key, 6)
    for dim, parts in cuts:
        draws = jnp.exp(jax.random.uniform(jax.random.fold_in(own, dim), (parts,), jnp.float32, least / len(cuts), top_value / len(cuts)))
        gain = gain * jnp.repeat(draws, extent[dim] // parts).reshape([-1 if axis == dim else 1 for axis in range(len(extent))])
    return gain


def bell_draw(key, dims, scale, reach, split=(), held_as=jnp.bfloat16):
    result = jax.random.normal(key, dims, jnp.float32) * scale
    if len(split) > 0:
        result = level_of(key, dims, split, -0.22, 0.18) * result
    return jnp.clip(result, min=-reach, max=reach).astype(held_as)


def setup_inputs(seed: int = 0) -> dict:
    splits = jax.random.split(jax.random.key(seed), 5)
    return {
        "solutions": bell_draw(splits[0], (TSL, SPINCOL, SITES, 2 * NVEC), 1.0, 6.0, ((0, 2), (2, 16))),
        "noise": plant(jax.random.randint(splits[1], (TSL, NVEC, SPINCOL, SITES), 0, 4), jax.random.fold_in(splits[1], 1), 0, 3).astype(jnp.int32),
        "momenta": plant(jax.random.randint(splits[2], (MOMS, 3), -2, 3), jax.random.fold_in(splits[2], 1), -2, 2).astype(jnp.int32),
        "pairs": plant(jax.random.randint(splits[3], (NPAIRS, 2), 0, TSL), jax.random.fold_in(splits[3], 1), 0, TSL - 1).astype(jnp.int32),
    }


def phase_weights(noise_block, momenta, coords):
    qdotx = momenta[:, 0:1] * coords[0][None, :] + momenta[:, 1:2] * coords[1][None, :] + momenta[:, 2:3] * coords[2][None, :]
    index = (EXTENT // 4 * noise_block[None, :, :, :] + qdotx[:, None, None, :]) % EXTENT
    angle = index.astype(jnp.float32) * jnp.float32(2.0 * math.pi / EXTENT)
    rows = momenta.shape[0] * noise_block.shape[0]
    cols = noise_block.shape[1] * noise_block.shape[2]
    weight_re = jnp.cos(angle).astype(jnp.bfloat16).reshape(rows, cols)
    weight_im = (-jnp.sin(angle)).astype(jnp.bfloat16).reshape(rows, cols)
    return (weight_re, weight_im)

def site_coords(first, count):
    glob = first + jnp.arange(count, dtype=jnp.int32)
    return (glob % EXTENT, glob // EXTENT % EXTENT, glob // (EXTENT * EXTENT))

def slice_field(vectors, sources, momenta):
    block = min(1024, SITES)
    nblocks = SITES // block

    def one_block(step, total):
        first = (step * block).astype(jnp.int32)
        noise_block = lax.dynamic_slice_in_dim(sources, first, block, 2)
        vec_block = lax.dynamic_slice_in_dim(vectors, first, block, 1)
        weight_re, weight_im = phase_weights(noise_block, momenta, site_coords(first, block))
        stacked = vec_block.reshape(SPINCOL * block, 2 * NVEC)
        left = jnp.dot(weight_re, stacked, preferred_element_type=jnp.float32)
        right = jnp.dot(weight_im, stacked, preferred_element_type=jnp.float32)
        real_part = left[:, :NVEC] - right[:, NVEC:]
        imag_part = left[:, NVEC:] + right[:, :NVEC]
        return total + jnp.stack([real_part, imag_part], 0)
    start = jnp.zeros((2, MOMS * NVEC, NVEC), jnp.float32)
    total = lax.fori_loop(0, nblocks, one_block, start)
    return total.reshape(2, MOMS, NVEC, NVEC)

def reference(solutions, noise, momenta, pairs):
    scale = 1.0 / math.sqrt(SPINCOL * SITES)
    fields = [slice_field(solutions[t], noise[t], momenta) * scale for t in range(TSL)]
    mesons = jnp.stack(fields, 0)
    sink = mesons[pairs[:, 1]]
    source = mesons[pairs[:, 0]]
    real_part = lax.optimization_barrier(jnp.sum(sink[:, 0] * source[:, 0] + sink[:, 1] * source[:, 1], axis=(2, 3)))
    imag_part = lax.optimization_barrier(jnp.sum(sink[:, 1] * source[:, 0] - sink[:, 0] * source[:, 1], axis=(2, 3)))
    correlators = jnp.stack([real_part, imag_part], 1) / NVEC
    return (mesons, correlators)
```

```python
import functools
import math

import jax
import jax.numpy as jnp
from jax import lax
from jax.experimental import pallas as pl
from jax.experimental.pallas import tpu as pltpu
from jax.sharding import PartitionSpec as P

EXTENT = 48
BLOCK = 64
LANES = 128
NCOMP = 5
HELD = (1.62322, 1.13025)
GAIN = (1.624206057120357, 1.1324218363011367)
MESH = pl.DeviceIdType.MESH
F32 = jnp.float32
BF16 = jnp.bfloat16


def fdiv(value, n):
    return jnp.floor((value + 0.5) * F32(1.0 / n))


def turn(value):
    return (value - fdiv(value, EXTENT) * EXTENT) * F32(2.0 * math.pi / EXTENT)


def iota(shape, axis):
    return lax.broadcasted_iota(jnp.int32, shape, axis)


def column(ref, row, size):
    line = jnp.broadcast_to(ref[row:row + 1, :size].astype(F32), (size, size))
    return jnp.sum(jnp.where(iota((size, size), 0) == iota((size, size), 1), line, F32(0.0)), axis=1, keepdims=True)


def coefficients(mom_ref, mp, offset, ngroup, kpad, scale):
    shape = (mp, kpad)
    lane = iota(shape, 1).astype(F32)
    part = fdiv(lane, ngroup)
    group = lane - part * ngroup
    rowslot = fdiv(group, NCOMP)
    comp = group - rowslot * NCOMP
    blk = fdiv(rowslot, 2)
    slot = rowslot - blk * 2
    row = fdiv(offset + blk * BLOCK, EXTENT) + slot
    zz = fdiv(row, EXTENT)
    yy = row - zz * EXTENT
    qx = jnp.broadcast_to(column(mom_ref, 0, mp), shape)
    qy = jnp.broadcast_to(column(mom_ref, 1, mp), shape)
    qz = jnp.broadcast_to(column(mom_ref, 2, mp), shape)
    angle = turn(qy * yy + qz * zz)
    c, s = jnp.cos(angle), jnp.sin(angle)
    side = jnp.where(qx < 0, F32(-1.0), F32(1.0))
    level = jnp.abs(qx)
    own = fdiv(comp + 1, 2)
    gain = jnp.where(own == 0, F32(scale), jnp.where(own == 1, F32(scale / GAIN[0]), F32(scale / GAIN[1])))
    gain = jnp.where((own == level) & (part < 3), gain, F32(0.0))
    is_sin = (comp == 2) | (comp == 4)
    a = jnp.where(is_sin, -side * s, c) * gain
    b = jnp.where(is_sin, side * c, s) * gain
    both = jnp.concatenate([a, b], axis=0)
    high = both.astype(BF16)
    low = (both - high.astype(F32)).astype(BF16)
    third = iota(both.shape, 1) >= 2 * ngroup
    return jnp.where(third, low.astype(F32), high.astype(F32)).astype(BF16)


def kernel(dims, mom_ref, pair_ref, noise_hbm, sol_hbm, mes_ref, tr_ref,
           raw, sol, momp, cmat, xtab, mask, field, sbuf, hbuf, qbuf, rcore, ry, rz, xb, ps,
           in_sem, cs, cr, ys, yr, zs, zr, xs, xr, pss, psr):
    nspace, nslices, rows, nvec, spincol, moms, scale = dims
    nz = nspace // 4
    ntile = raw.shape[0]
    nblk = ntile * 2
    ngroup = nblk * 2 * NCOMP
    mp = cmat.shape[0] // 2
    fs = nvec + 8
    me = lax.axis_index("space")
    slice_id = lax.axis_index("tm")
    core = lax.rem(me, 2)
    yy = lax.rem(me // 2, 2)
    zz = me // 4
    first = me * (ntile * LANES)

    barrier = pltpu.get_barrier_semaphore()
    for o in range(1, nspace):
        pl.semaphore_signal(barrier, inc=1, device_id={"space": lax.rem(me + o, nspace)}, device_id_type=MESH)
    for o in range(1, nslices):
        pl.semaphore_signal(barrier, inc=1, device_id={"tm": lax.rem(slice_id + o, nslices)}, device_id_type=MESH)

    def noise_copy(k):
        return pltpu.make_async_copy(noise_hbm.at[:, :, pl.ds(k * LANES, LANES)], raw.at[k], in_sem.at[0, k])

    def sol_copy(k):
        return pltpu.make_async_copy(sol_hbm.at[:, pl.ds(k * LANES, LANES), :], sol.at[k], in_sem.at[1, k])

    for k in range(ntile):
        noise_copy(k).start()
        sol_copy(k).start()

    offset = first.astype(F32)
    momp[...] = jnp.zeros_like(momp)
    momp[:3, :moms] = mom_ref[...].astype(F32)
    cmat[...] = coefficients(momp, mp, offset, ngroup, cmat.shape[1], scale)
    for blk in range(nblk):
        lane = iota((16, LANES), 1).astype(F32)
        site = lane - jnp.where(lane >= BLOCK, F32(BLOCK), F32(0.0))
        x = offset + F32(blk * BLOCK) + site
        for k in range(2):
            angle = turn(x * F32(k + 1))
            xtab[blk * 4 + 2 * k] = (jnp.cos(angle) * F32(HELD[k])).astype(BF16)
            xtab[blk * 4 + 2 * k + 1] = (jnp.sin(angle) * F32(HELD[k])).astype(BF16)
        t = iota((LANES, LANES), 0).astype(F32)
        t = t - jnp.where(t >= BLOCK, F32(BLOCK), F32(0.0))
        start = offset + F32(blk * BLOCK)
        mask[blk] = jnp.where(fdiv(start + t, EXTENT) == fdiv(start, EXTENT), F32(1.0), F32(0.0)).astype(BF16)

    low = iota((nvec, LANES), 1) < BLOCK
    rsign = jnp.where(iota((LANES, LANES), 1) < nvec, F32(-1.0), F32(1.0)).astype(BF16)

    def spread(v, n):
        return jnp.concatenate([v] * n, axis=0)

    for k in range(ntile):
        noise_copy(k).wait()
        sol_copy(k).wait()
        for h in range(2):
            blk = 2 * k + h
            xs_rows = [spread(xtab[blk * 4 + c], nvec // 16) for c in range(4)]
            keep = mask[blk]
            total = None
            for p in range(spincol // 2):
                ka = raw[k, 2 * p]
                kb = raw[k, 2 * p + 1]
                if h == 0:
                    kk = jnp.where(low, ka, pltpu.roll(kb, BLOCK, 1))
                else:
                    kk = jnp.where(low, pltpu.roll(ka, BLOCK, 1), kb)
                kf = kk.astype(F32)
                re = jnp.where(kk == 3, F32(0.0), F32(1.0) - kf).astype(BF16)
                im = jnp.where(kk == 0, F32(0.0), kf - F32(2.0)).astype(BF16)
                parts = [jnp.concatenate([re, im], axis=1)]
                for c in range(4):
                    parts.append(jnp.concatenate([re * xs_rows[c], im * xs_rows[c]], axis=1))
                lhs = jnp.concatenate(parts, axis=0)
                v = jnp.concatenate([sol[k, 2 * p, h * BLOCK:(h + 1) * BLOCK, :],
                                     sol[k, 2 * p + 1, h * BLOCK:(h + 1) * BLOCK, :]], axis=0)
                rv = pltpu.roll(v, nvec, 1) * rsign
                v0, rv0 = v * keep, rv * keep
                rhs = jnp.concatenate([jnp.concatenate([v0, v - v0], axis=1),
                                       jnp.concatenate([rv0, rv - rv0], axis=1)], axis=0)
                prod = jnp.dot(lhs, rhs, preferred_element_type=F32)
                total = prod if total is None else total + prod
            for slot in range(2):
                for c in range(NCOMP):
                    g = (blk * 2 + slot) * NCOMP + c
                    field[g * fs:g * fs + nvec, :] = total[c * nvec:(c + 1) * nvec, slot * LANES:(slot + 1) * LANES]

    def remote(src, dst, ssem, rsem, where):
        return pltpu.make_async_remote_copy(src_ref=src, dst_ref=dst, send_sem=ssem, recv_sem=rsem,
                                            device_id=where, device_id_type=MESH)

    used = pl.ds(0, moms)

    def peer(m):
        if nz & (nz - 1):
            return lax.rem(zz + m, nz)
        out, bit = 0, 1
        while bit < nz:
            digit = lax.rem(zz // bit, 2)
            out = out + bit * (1 - digit if m & bit else digit)
            bit *= 2
        return out

    core_peer = {"space": me + 1 - 2 * core}
    y_peer = {"space": me + 2 - 4 * yy}
    order = list(range(nz - 1, -1, -1))

    def core_copy(m, far):
        return remote(sbuf.at[far, m, 1 - core, :, used], rcore.at[far, m, :, used], cs.at[far, m], cr.at[far, m],
                      core_peer)

    def y_copy(m):
        return remote(hbuf.at[m, :, used], ry.at[m, :, used], ys.at[m], yr.at[m], y_peer)

    def z_copy(m):
        return remote(qbuf.at[m, :, used], rz.at[m, :, used], zs.at[m], zr.at[m],
                      {"space": peer(m) * 4 + yy * 2 + core})

    def x_copy(o):
        return remote(xb.at[slice_id, :, used], xb.at[slice_id, :, used], xs.at[o - 1], xr.at[o - 1],
                      {"tm": lax.rem(slice_id + o, nslices)})

    def p_copy(o):
        return remote(ps.at[me], ps.at[me], pss.at[o - 1], psr.at[o - 1],
                      {"space": lax.rem(me + o, nspace)})

    osign = jnp.where(iota((mp, LANES), 1) < nvec, F32(1.0), F32(-1.0))
    kpad = cmat.shape[1]

    def compute(m, far):
        base = peer(m) * (4 * rows) + (1 - yy if far else yy) * (2 * rows)
        coef = cmat[...]
        for pair in range(rows):
            xf = jnp.concatenate([field[pl.ds(base + 2 * pair + e, ngroup, stride=fs), :] for e in range(2)], axis=1)
            high = xf.astype(BF16)
            rest = (xf - high.astype(F32)).astype(BF16)
            stack = [high, rest, high]
            if kpad > 3 * ngroup:
                stack.append(jnp.zeros((kpad - 3 * ngroup, 2 * LANES), BF16))
            res = jnp.dot(coef, jnp.concatenate(stack, axis=0), preferred_element_type=F32)
            for e in range(2):
                idx = 2 * pair + e
                a = res[:mp, e * LANES:(e + 1) * LANES]
                b = res[mp:, e * LANES:(e + 1) * LANES]
                sbuf[far, m, idx // rows, idx % rows] = a + pltpu.roll(b, nvec, 1) * osign

    started = False
    for far in (1, 0):
        for m in order:
            compute(m, far)
            if not started:
                pl.semaphore_wait(barrier, nspace - 1 + nslices - 1)
                started = True
            core_copy(m, far).start()

    for m in order:
        core_copy(m, 1).wait_recv()
        hbuf[m] = sbuf[1, m, core] + rcore[1, m]
        y_copy(m).start()
    for m in order[:-1]:
        core_copy(m, 0).wait_recv()
        y_copy(m).wait_recv()
        qbuf[m] = (sbuf[0, m, core] + rcore[0, m]) + ry[m]
        z_copy(m).start()
    core_copy(0, 0).wait_recv()
    y_copy(0).wait_recv()
    total = (sbuf[0, 0, core] + rcore[0, 0]) + ry[0]
    for m in order[:-1]:
        z_copy(m).wait_recv()
        total = total + rz[m]
    xb[slice_id] = total
    for o in range(1, nslices):
        x_copy(o).start()
    for r in range(rows):
        mes_ref[0, r] = total[r, :moms, :nvec]
        mes_ref[1, r] = pltpu.roll(total[r], nvec, 1)[:moms, :nvec]
    for o in range(1, nslices):
        x_copy(o).wait_recv()

    prods = [None] * (nslices * nslices)
    for w in range(nslices):
        for u in range(w + 1):
            re = im = None
            for r in range(rows):
                mw, mu = xb[w, r], xb[u, r]
                part = mw * mu
                re = part if re is None else re + part
                if u < w:
                    part = mw * (pltpu.roll(mu, nvec, 1) * osign)
                    im = part if im is None else im + part
            prods[w * nslices + u] = re
            if u < w:
                prods[u * nslices + w] = -im
    table = jnp.concatenate(prods, axis=0)
    found = lax.dot_general(jnp.ones((8, LANES), F32), table, (((1,), (1,)), ((), ())),
                            precision=lax.Precision.HIGHEST, preferred_element_type=F32)
    ps[me] = found[0:1]
    for o in range(1, nspace):
        p_copy(o).start()
    for o in range(1, nspace):
        p_copy(o).wait_recv()
    tot = ps[0]
    for d in range(1, nspace):
        tot = tot + ps[d]
    tot = tot * F32(1.0 / nvec)
    npair = pair_ref.shape[1]
    source, sink = column(pair_ref, 0, npair), column(pair_ref, 1, npair)
    high, small = jnp.maximum(source, sink), jnp.minimum(source, sink)
    turned = jnp.where(sink > source, F32(1.0), jnp.where(sink < source, F32(-1.0), F32(0.0)))
    real = jnp.zeros((npair, mp), F32)
    imag = jnp.zeros((npair, mp), F32)
    for k in range(nslices * nslices):
        line = tot[:, k * mp:(k + 1) * mp]
        real = real + jnp.where(high * nslices + small == k, F32(1.0), F32(0.0)) * line
        imag = imag + jnp.where(small * nslices + high == k, turned, F32(0.0)) * line
    tr_ref[:, 0, :] = real[:, :moms]
    tr_ref[:, 1, :] = imag[:, :moms]

    for m in order:
        core_copy(m, 0).wait_send()
        core_copy(m, 1).wait_send()
        y_copy(m).wait_send()
    for m in order[:-1]:
        z_copy(m).wait_send()
    for o in range(1, nslices):
        x_copy(o).wait_send()
    for o in range(1, nspace):
        p_copy(o).wait_send()


def local(solutions, noise, momenta, pairs):
    _, spincol, sites, width = solutions.shape
    nvec = width // 2
    moms = momenta.shape[0]
    nspace = lax.axis_size("space")
    nslices = lax.axis_size("tm")
    nz = nspace // 4
    rows = nvec // nspace
    scale = 1.0 / math.sqrt(spincol * sites * nspace)
    ntile = sites // LANES
    ngroup = ntile * 4 * NCOMP
    kpad = -(-3 * ngroup // LANES) * LANES
    mp = -(-moms // 16) * 16
    blk = (rows, mp, width)
    dims = (nspace, nslices, rows, nvec, spincol, moms, scale)
    dma = pltpu.SemaphoreType.DMA
    vmem = pl.BlockSpec(memory_space=pltpu.VMEM)
    hbm = pl.BlockSpec(memory_space=pl.ANY)
    mesons, correlators = pl.pallas_call(
        functools.partial(kernel, dims),
        out_shape=(jax.ShapeDtypeStruct((2, rows, moms, nvec), F32),
                   jax.ShapeDtypeStruct((pairs.shape[0], 2, moms), F32)),
        in_specs=[vmem, vmem, hbm, hbm],
        out_specs=(vmem, vmem),
        scratch_shapes=[
            pltpu.VMEM((ntile, spincol, nvec, LANES), jnp.int32),
            pltpu.VMEM((ntile, spincol, LANES, width), BF16),
            pltpu.VMEM((8, -(-mp // LANES) * LANES), F32),
            pltpu.VMEM((2 * mp, kpad), BF16),
            pltpu.VMEM((ntile * 8, 16, LANES), BF16),
            pltpu.VMEM((ntile * 2, LANES, LANES), BF16),
            pltpu.VMEM((ngroup * (nvec + 8), width), F32),
            pltpu.VMEM((2, nz, 2) + blk, F32),
            pltpu.VMEM((nz,) + blk, F32),
            pltpu.VMEM((nz,) + blk, F32),
            pltpu.VMEM((2, nz) + blk, F32),
            pltpu.VMEM((nz,) + blk, F32),
            pltpu.VMEM((nz,) + blk, F32),
            pltpu.VMEM((nslices,) + blk, F32),
            pltpu.VMEM((nspace, 1, nslices * nslices * mp), F32),
            dma((2, ntile)),
            dma((2, nz)), dma((2, nz)),
            dma((nz,)), dma((nz,)),
            dma((nz,)), dma((nz,)),
            dma((nslices - 1,)), dma((nslices - 1,)),
            dma((nspace - 1,)), dma((nspace - 1,)),
        ],
        compiler_params=pltpu.CompilerParams(collective_id=0, has_side_effects=True, vmem_limit_bytes=60 * 2**20),
    )(momenta.T, pairs.T, noise[0].transpose(1, 0, 2), solutions[0])
    return (mesons.transpose(0, 2, 1, 3)[None], correlators)


def solution(mesh):
    in_specs = (P("tm", None, "space", None), P("tm", None, None, "space"), P(), P("tm", None))
    out_specs = (P("tm", None, None, "space", None), P("tm", None, None))
    return jax.shard_map(local, mesh=mesh, in_specs=in_specs, out_specs=out_specs, check_vma=False)
```
